32 devices in a mesh: groups: 2 (over x), aux: 16 (over z, y, core).
Axes of the slice: x: 2, y: 2, z: 4, core: 2. Of those that a mesh axis runs over, the one named last changes fastest.
Arguments:
- slabs: bfloat16 [8000, 23040], P(('groups', 'aux')), parts along dimension 0, may hold values from -2 to 2
- rdm: bfloat16 [1800, 900], P('groups'), parts along dimension 0, as said below
- orbital_energy: float32 [1536], P('groups'), parts along dimension 0, may hold values from 0.5 to 3
- pair_blocks: int32 [32, 2], P('groups'), parts along dimension 0, may hold values from 0 to 15, as said below
Outputs:
- pair_energy: float32 [1536, 48], P(('groups', 'aux')), parts along dimension 0
- window_energy: float32 [2], P('groups'), parts along dimension 0
The draws below stay inside these ranges and needn't reach their ends.
There are 2 independent parts, one for each index of `groups`. The reference program is written for one: setup_inputs(seed, part) draws one part's arguments, and reference() takes and returns one part's arrays. A program takes and returns all parts, laid end to end along the dimension named above; each array names one. Nothing has to cross between parts.
Inputs may be any that keep to these rules, and one draw needn't show every extreme that they name: `pair_blocks`: each row (p, q) has p <= q, and no two rows are equal. `rdm`: symmetric.
All inputs are finite; a program needn't handle non-finite values.
Results may differ from the reference program's by a relative error of at most 0.002.
Values may be sent and summed in bfloat16 or wider, within the bound.
A program may use at most 128 MiB of HBM per device.

```python
import math
import jax
import jax.numpy as jnp
from jax import lax

NAUX = 4000
NACT = 30
VBLK = 48
NBLK = 16
NVIR = 768
N_AUX = 16


def draw_rdm(key, part):
    order = NACT * NACT
    first, second = jax.random.split(jax.random.fold_in(key, 11))
    base = jax.random.normal(first, (order, order), jnp.float32)
    spread = 0.5
    diagonal = jax.random.uniform(second, (order,), jnp.float32, 1.0, 2.0)
    symmetric = (base + base.T) * (spread / math.sqrt(2.0))
    return ((jnp.diag(diagonal) + symmetric) / order).astype(jnp.bfloat16)


def draw_pair_blocks(key, part):
    count = NBLK * (NBLK + 1) // 2
    chosen = jax.random.permutation(jax.random.fold_in(key, 23), count)[:N_AUX].astype(jnp.int32)
    rows = jnp.arange(NBLK, dtype=jnp.int32)
    starts = rows * NBLK - rows * (rows - 1) // 2
    first = jnp.sum((chosen[:, None] >= starts[None, 1:]).astype(jnp.int32), axis=1)
    begin = first * NBLK - first * (first - 1) // 2
    second = first + chosen - begin
    return jnp.stack([first, second], axis=1).astype(jnp.int32)


def levels(rng, shape, cuts, low, largest):
    loudness, own = 1.0, jax.random.fold_in(rng, 6)
    for position, shards_of in cuts:
        heights = jnp.exp(jax.random.uniform(jax.random.fold_in(own, position), (shards_of,), jnp.float32, low / len(cuts), largest / len(cuts)))
        loudness = loudness * jnp.repeat(heights, shape[position] // shards_of).reshape([-1 if axis == position else 1 for axis in range(len(shape))])
    return loudness


def centred(own_key, dims, width, reach, pieces=(), kind=jnp.bfloat16):
    entries = jax.random.normal(own_key, dims, jnp.float32) * width
    if len(pieces) > 0:
        entries = levels(own_key, dims, pieces, -0.22, 0.18) * entries
    return jnp.clip(entries, min=-reach, max=reach).astype(kind)


def setup_inputs(seed: int = 0, part: int = 0) -> dict:
    streams_of = jax.random.split(jax.random.key(seed), 5)
    part_splits = jax.random.split(jax.random.fold_in(streams_of[4], part), 5)
    slabs = centred(part_splits[0], (NAUX, NVIR * NACT), (1 / NAUX ** 0.25), 2.0, ((0, 16),))
    rdm = draw_rdm(jax.random.fold_in(jax.random.fold_in(streams_of[4], part), 71), part)
    orbital_energy = jnp.clip(jnp.exp(jax.random.uniform(part_splits[2], (NVIR,), jnp.float32, math.log(0.5), math.log(3.0))), 0.5, 3.0)
    pair_blocks = draw_pair_blocks(jax.random.fold_in(jax.random.fold_in(streams_of[4], part), 71), part)
    return dict(slabs=slabs, rdm=rdm, orbital_energy=orbital_energy, pair_blocks=pair_blocks)


def reference(slabs, rdm, orbital_energy, pair_blocks):
    blocked = slabs.reshape(NAUX, NBLK, VBLK * NACT)
    energy_table = orbital_energy.reshape(NBLK, VBLK)

    def one_pair(blocks):
        row_part = blocked[:, blocks[0]]
        col_part = blocked[:, blocks[1]]
        integrals = lax.dot_general(row_part, col_part, (((0,), (0,)), ((), ())), preferred_element_type=jnp.float32).astype(jnp.bfloat16)
        reordered = integrals.reshape(VBLK, NACT, VBLK, NACT).transpose(0, 2, 1, 3).reshape(VBLK * VBLK, NACT * NACT)
        contracted = jnp.dot(reordered, rdm, preferred_element_type=jnp.float32)
        paired = jnp.sum(contracted * reordered.astype(jnp.float32), axis=1).reshape(VBLK, VBLK)
        energy = -paired / (energy_table[blocks[0]][:, None] + energy_table[blocks[1]][None, :])
        weight = jnp.where(blocks[0] == blocks[1], jnp.float32(1.0), jnp.float32(2.0))
        return energy, weight * jnp.sum(energy)

    energies, totals = lax.map(one_pair, pair_blocks)
    mean_energy = jnp.sum(totals) / (VBLK * VBLK * N_AUX)
    return energies.reshape(N_AUX * VBLK, VBLK), mean_energy.reshape(1)
```

```python
import functools

import jax
import jax.numpy as jnp
from jax import lax
from jax.experimental import pallas as pl
from jax.experimental.pallas import tpu as pltpu
from jax.sharding import PartitionSpec as P

NACT = 30
VBLK = 48
LANE = 128
HALF = 64
TPAD = 32
WIDTH = VBLK * NACT
WINDOW = -(-(WIDTH + LANE - 32) // LANE) * LANE
UPAIRS = NACT // 2
BF16 = jnp.bfloat16
F32 = jnp.float32


def window_start(block):
    return (block * WIDTH) // LANE * LANE


def gather_body(pairs_ref, in_ref, out_ref):
    out_ref[0] = in_ref[...]


def gather(slabs, pair_blocks):
    rows = slabs.shape[0]
    n = pair_blocks.shape[0]
    return pl.pallas_call(
        gather_body,
        grid_spec=pltpu.PrefetchScalarGridSpec(
            num_scalar_prefetch=1,
            grid=(n, 2),
            in_specs=[
                pl.BlockSpec(
                    (pl.Element(rows), pl.Element(WINDOW)),
                    lambda d, j, pairs: (0, pl.multiple_of(window_start(pairs[d, j]), LANE)),
                )
            ],
            out_specs=pl.BlockSpec((1, rows, WINDOW), lambda d, j, pairs: (d, 0, j)),
        ),
        out_shape=jax.ShapeDtypeStruct((n, rows, 2 * WINDOW), BF16),
        name="gather_blocks",
    )(pair_blocks, slabs)


def exchange_body(n, g_ref, out_ref, recv, acc, local_sem, send_sem, recv_sem):
    me = lax.axis_index("aux")

    barrier = pltpu.get_barrier_semaphore()

    @pl.loop(1, n)
    def _(s):
        pl.semaphore_signal(
            barrier, inc=1, device_id={"aux": lax.rem(me + s, n)}, device_id_type=pl.DeviceIdType.MESH
        )

    own = pltpu.make_async_copy(g_ref.at[me], recv.at[me], local_sem)
    own.start()
    pl.semaphore_wait(barrier, n - 1)

    def send(s):
        to = lax.rem(me + s, n)
        return pltpu.make_async_remote_copy(
            src_ref=g_ref.at[to],
            dst_ref=recv.at[me],
            send_sem=send_sem.at[to],
            recv_sem=recv_sem.at[me],
            device_id={"aux": to},
            device_id_type=pl.DeviceIdType.MESH,
        )

    @pl.loop(1, n)
    def _(s):
        send(s).start()

    acc[...] = jnp.zeros_like(acc)
    own.wait()
    tile = 256

    def add(source):
        @pl.loop(0, WINDOW // tile)
        def _(m):
            at = pl.ds(pl.multiple_of(m * tile, tile), tile)
            acc[at, :] += lax.dot_general(
                recv[source, :, at],
                recv[source, :, WINDOW:],
                (((0,), (0,)), ((), ())),
                preferred_element_type=F32,
            )

    add(me)

    @pl.loop(1, n)
    def _(s):
        source = lax.rem(me + n - s, n)
        pltpu.make_async_remote_copy(
            src_ref=g_ref.at[source],
            dst_ref=recv.at[source],
            send_sem=send_sem.at[source],
            recv_sem=recv_sem.at[source],
            device_id={"aux": source},
            device_id_type=pl.DeviceIdType.MESH,
        ).wait_recv()
        add(source)

    out_ref[...] = acc[...].astype(BF16)

    @pl.loop(1, n)
    def _(s):
        send(s).wait_send()


def exchange(g):
    n, rows, both = g.shape
    return pl.pallas_call(
        functools.partial(exchange_body, n),
        out_shape=jax.ShapeDtypeStruct((WINDOW, WINDOW), BF16),
        in_specs=[pl.BlockSpec(memory_space=pl.ANY)],
        out_specs=pl.BlockSpec(memory_space=pltpu.VMEM),
        scratch_shapes=[
            pltpu.VMEM((n, rows, both), BF16),
            pltpu.VMEM((WINDOW, WINDOW), F32),
            pltpu.SemaphoreType.DMA,
            pltpu.SemaphoreType.DMA((n,)),
            pltpu.SemaphoreType.DMA((n,)),
        ],
        compiler_params=pltpu.CompilerParams(
            collective_id=0, has_side_effects=True, vmem_limit_bytes=56 * 2**20
        ),
        name="exchange_blocks",
    )(g)


def pair_body(i_ref, prow_ref, pcol_ref, r_ref, out_ref, x_ref):
    tile = 256

    @pl.loop(0, VBLK * TPAD // tile)
    def _(m):
        at = pl.ds(pl.multiple_of(m * tile, tile), tile)
        picked = jnp.dot(prow_ref[at, :], i_ref[...], preferred_element_type=F32).astype(BF16)
        x_ref[at, :] = jnp.dot(picked, pcol_ref[...], preferred_element_type=F32).astype(BF16)

    half = UPAIRS * TPAD

    def stacked(a):
        rows = pl.ds(pl.multiple_of(a * TPAD, TPAD), TPAD)
        return jnp.concatenate([x_ref[rows, u * LANE : (u + 1) * LANE] for u in range(UPAIRS)], axis=0)

    low = lax.broadcasted_iota(jnp.int32, (half, LANE), 1) < HALF

    @pl.loop(0, VBLK // 2)
    def _(m):
        first, second = stacked(2 * m), stacked(2 * m + 1)
        x = jnp.concatenate([first, second], axis=1)
        z0 = jnp.dot(r_ref[:, :half], x, preferred_element_type=F32)
        z1 = jnp.dot(r_ref[:, half:], x, preferred_element_type=F32)
        sums = []
        for k, part in enumerate((first, second)):
            lanes = slice(k * LANE, (k + 1) * LANE)
            xf = part.astype(F32)
            turned = pltpu.roll(xf, HALF, 1)
            b0 = jnp.where(low, xf, turned)
            b1 = jnp.where(low, turned, xf)
            t0 = jnp.where(low, z0[:half, lanes], z1[:half, lanes])
            t1 = jnp.where(low, z0[half:, lanes], z1[half:, lanes])
            sums.append(jnp.sum(t0 * b0 + t1 * b1, axis=0, keepdims=True))
        out_ref[m] = jnp.concatenate(sums, axis=0)


def pair_sums(integrals, prow, pcol, r):
    return pl.pallas_call(
        pair_body,
        out_shape=jax.ShapeDtypeStruct((VBLK // 2, 2, LANE), F32),
        in_specs=[pl.BlockSpec(memory_space=pltpu.VMEM)] * 4,
        out_specs=pl.BlockSpec(memory_space=pltpu.VMEM),
        scratch_shapes=[pltpu.VMEM((VBLK * TPAD, UPAIRS * LANE), BF16)],
        compiler_params=pltpu.CompilerParams(vmem_limit_bytes=48 * 2**20),
        name="pair_sums",
    )(integrals, prow, pcol, r)


def selectors(row_block, col_block):
    row_off = row_block * WIDTH - window_start(row_block)
    col_off = col_block * WIDTH - window_start(col_block)
    at = jnp.arange(VBLK * TPAD)
    a, t = at // TPAD, at % TPAD
    want = jnp.where(t < NACT, row_off + a * NACT + t, -1)
    prow = (want[:, None] == jnp.arange(WINDOW)[None, :]).astype(BF16)
    j = jnp.arange(UPAIRS * LANE)
    u, b = 2 * (j // LANE) + (j % LANE) // HALF, j % HALF
    want = jnp.where(b < VBLK, col_off + b * NACT + u, -1)
    pcol = (jnp.arange(WINDOW)[:, None] == want[None, :]).astype(BF16)
    return prow, pcol


def ordered_rdm(rdm):
    half = UPAIRS * TPAD
    j = jnp.arange(2 * half)
    u, t = 2 * ((j % half) // TPAD) + j // half, j % TPAD
    want = jnp.where(t < NACT, t * NACT + u, -1)
    pick = (want[:, None] == jnp.arange(NACT * NACT)[None, :]).astype(BF16)
    once = lax.dot_general(pick, rdm, (((1,), (1,)), ((), ())), preferred_element_type=F32).astype(BF16)
    return lax.dot_general(once, pick, (((1,), (1,)), ((), ())), preferred_element_type=F32).astype(BF16)


def per_device(slabs, rdm, orbital_energy, pair_blocks):
    position = lax.axis_index("aux")
    row_block = pair_blocks[position, 0]
    col_block = pair_blocks[position, 1]
    prow, pcol = selectors(row_block, col_block)
    r = ordered_rdm(rdm)
    integrals = exchange(gather(slabs, pair_blocks))
    raw = pair_sums(integrals, prow, pcol, r)
    paired = raw.reshape(VBLK, 2, HALF).sum(axis=1)[:, :VBLK]
    energy_rows = lax.dynamic_slice_in_dim(orbital_energy, row_block * VBLK, VBLK)
    energy_cols = lax.dynamic_slice_in_dim(orbital_energy, col_block * VBLK, VBLK)
    energy = -paired / (energy_rows[:, None] + energy_cols[None, :])
    weight = jnp.where(row_block == col_block, F32(1.0), F32(2.0))
    total = lax.psum(weight * jnp.sum(energy), "aux")
    mean_energy = total / (VBLK * VBLK * lax.axis_size("aux"))
    return (energy, mean_energy.reshape(1))


def solution(mesh):
    return jax.shard_map(
        per_device,
        mesh=mesh,
        in_specs=(P(("groups", "aux"), None), P("groups", None), P("groups"), P("groups", None)),
        out_specs=(P(("groups", "aux"), None), P("groups")),
        check_vma=False,
    )
```

```python
import functools

import jax
import jax.numpy as jnp
from jax import lax
from jax.experimental import pallas as pl
from jax.experimental.pallas import tpu as pltpu
from jax.sharding import PartitionSpec as P

NACT = 30
VBLK = 48
LANE = 128
HALF = 64
TPAD = 32
WIDTH = VBLK * NACT
WINDOW = -(-(WIDTH + LANE - 32) // LANE) * LANE
UPAIRS = NACT // 2
BF16 = jnp.bfloat16
F32 = jnp.float32


def window_start(block):
    return (block * WIDTH) // LANE * LANE


def gather_body(pairs_ref, in_ref, out_ref):
    out_ref[0] = in_ref[...]


def gather(slabs, pair_blocks):
    rows = slabs.shape[0]
    n = pair_blocks.shape[0]
    return pl.pallas_call(
        gather_body,
        grid_spec=pltpu.PrefetchScalarGridSpec(
            num_scalar_prefetch=1,
            grid=(n, 2),
            in_specs=[
                pl.BlockSpec(
                    (pl.Element(rows), pl.Element(WINDOW)),
                    lambda d, j, pairs: (0, pl.multiple_of(window_start(pairs[d, j]), LANE)),
                )
            ],
            out_specs=pl.BlockSpec((1, rows, WINDOW), lambda d, j, pairs: (d, 0, j)),
        ),
        out_shape=jax.ShapeDtypeStruct((n, rows, 2 * WINDOW), BF16),
        name="gather_blocks",
    )(pair_blocks, slabs)


def exchange_body(size, g_ref, shift_ref, out_ref, recv, acc, local_sem, send_sem, recv_sem):
    position = lax.axis_index("aux")
    base = position // size * size
    me = position - base

    def device(member):
        return {"aux": base + member}

    barrier = pltpu.get_barrier_semaphore()

    @pl.loop(1, size)
    def _(s):
        pl.semaphore_signal(
            barrier, inc=1, device_id=device(lax.rem(me + s, size)), device_id_type=pl.DeviceIdType.MESH
        )

    own = pltpu.make_async_copy(g_ref.at[me], recv.at[me], local_sem)
    own.start()
    pl.semaphore_wait(barrier, size - 1)

    def send(s):
        to = lax.rem(me + s, size)
        return pltpu.make_async_remote_copy(
            src_ref=g_ref.at[to],
            dst_ref=recv.at[me],
            send_sem=send_sem.at[to],
            recv_sem=recv_sem.at[me],
            device_id=device(to),
            device_id_type=pl.DeviceIdType.MESH,
        )

    @pl.loop(1, size)
    def _(s):
        send(s).start()

    acc[...] = jnp.zeros_like(acc)
    own.wait()
    tile = 256

    def add(source):
        @pl.loop(0, WINDOW // tile)
        def _(m):
            at = pl.ds(pl.multiple_of(m * tile, tile), tile)
            acc[at, :] += lax.dot_general(
                recv[source, :, at],
                recv[source, :, WINDOW:],
                (((0,), (0,)), ((), ())),
                preferred_element_type=F32,
            )

    add(me)

    @pl.loop(1, size)
    def _(s):
        source = lax.rem(me + size - s, size)
        pltpu.make_async_remote_copy(
            src_ref=g_ref.at[source],
            dst_ref=recv.at[source],
            send_sem=send_sem.at[source],
            recv_sem=recv_sem.at[source],
            device_id=device(source),
            device_id_type=pl.DeviceIdType.MESH,
        ).wait_recv()
        add(source)

    shift = shift_ref[0]
    piece = 96

    @pl.loop(0, WIDTH // piece)
    def _(m):
        def from_row(offset):
            return acc[pl.ds(pl.multiple_of(m * piece + offset, 32), piece), :]

        low = jnp.where(shift == 0, from_row(0), from_row(32))
        high = jnp.where(shift == 64, from_row(64), from_row(96))
        out_ref[pl.ds(pl.multiple_of(m * piece, 32), piece), :] = jnp.where(shift < 64, low, high)

    @pl.loop(1, size)
    def _(s):
        send(s).wait_send()


def exchange(g, shift, identity):
    size, rows, both = g.shape
    return pl.pallas_call(
        functools.partial(exchange_body, size),
        out_shape=jax.ShapeDtypeStruct((WIDTH, WINDOW), F32),
        in_specs=[pl.BlockSpec(memory_space=pl.ANY), pl.BlockSpec(memory_space=pltpu.SMEM)],
        out_specs=pl.BlockSpec(memory_space=pltpu.VMEM),
        scratch_shapes=[
            pltpu.VMEM((size, rows, both), BF16),
            pltpu.VMEM((WINDOW, WINDOW), F32),
            pltpu.SemaphoreType.DMA,
            pltpu.SemaphoreType.DMA((size,)),
            pltpu.SemaphoreType.DMA((size,)),
        ],
        compiler_params=pltpu.CompilerParams(
            collective_id=identity, has_side_effects=True, vmem_limit_bytes=40 * 2**20
        ),
        cost_estimate=pl.CostEstimate(
            flops=200 * size * rows * WINDOW * WINDOW, bytes_accessed=2 * size * rows * both, transcendentals=0
        ),
        name=f"exchange_blocks_{identity}",
    )(g, shift)


def pair_body(i_ref, prow_ref, pcol_ref, r_ref, out_ref, x_ref):
    tile = 256

    @pl.loop(0, VBLK * TPAD // tile)
    def _(m):
        at = pl.ds(pl.multiple_of(m * tile, tile), tile)
        picked = jnp.dot(prow_ref[at, :], i_ref[...], preferred_element_type=F32).astype(BF16)
        x_ref[at, :] = jnp.dot(picked, pcol_ref[...], preferred_element_type=F32).astype(BF16)

    half = UPAIRS * TPAD

    def stacked(a):
        rows = pl.ds(pl.multiple_of(a * TPAD, TPAD), TPAD)
        return jnp.concatenate([x_ref[rows, u * LANE : (u + 1) * LANE] for u in range(UPAIRS)], axis=0)

    low = lax.broadcasted_iota(jnp.int32, (half, LANE), 1) < HALF

    @pl.loop(0, VBLK // 2)
    def _(m):
        first, second = stacked(2 * m), stacked(2 * m + 1)
        x = jnp.concatenate([first, second], axis=1)
        z0 = jnp.dot(r_ref[:, :half], x, preferred_element_type=F32)
        z1 = jnp.dot(r_ref[:, half:], x, preferred_element_type=F32)
        sums = []
        for k, part in enumerate((first, second)):
            lanes = slice(k * LANE, (k + 1) * LANE)
            xf = part.astype(F32)
            turned = pltpu.roll(xf, HALF, 1)
            b0 = jnp.where(low, xf, turned)
            b1 = jnp.where(low, turned, xf)
            t0 = jnp.where(low, z0[:half, lanes], z1[:half, lanes])
            t1 = jnp.where(low, z0[half:, lanes], z1[half:, lanes])
            sums.append(jnp.sum(t0 * b0 + t1 * b1, axis=0, keepdims=True))
        out_ref[m] = jnp.concatenate(sums, axis=0)


def pair_sums(integrals, prow, pcol, r):
    return pl.pallas_call(
        pair_body,
        out_shape=jax.ShapeDtypeStruct((VBLK // 2, 2, LANE), F32),
        in_specs=[pl.BlockSpec(memory_space=pltpu.VMEM)] * 4,
        out_specs=pl.BlockSpec(memory_space=pltpu.VMEM),
        scratch_shapes=[pltpu.VMEM((VBLK * TPAD, UPAIRS * LANE), BF16)],
        compiler_params=pltpu.CompilerParams(vmem_limit_bytes=48 * 2**20),
        name="pair_sums",
    )(integrals, prow, pcol, r)


def selectors(col_block):
    col_off = col_block * WIDTH - window_start(col_block)
    at = jnp.arange(VBLK * TPAD)
    a, t = at // TPAD, at % TPAD
    want = jnp.where(t < NACT, a * NACT + t, -1)
    prow = (want[:, None] == jnp.arange(WIDTH)[None, :]).astype(BF16)
    j = jnp.arange(UPAIRS * LANE)
    u, b = 2 * (j // LANE) + (j % LANE) // HALF, j % HALF
    want = jnp.where(b < VBLK, col_off + b * NACT + u, -1)
    pcol = (jnp.arange(WINDOW)[:, None] == want[None, :]).astype(BF16)
    return prow, pcol


def ordered_rdm(rdm):
    half = UPAIRS * TPAD
    j = jnp.arange(2 * half)
    u, t = 2 * ((j % half) // TPAD) + j // half, j % TPAD
    want = jnp.where(t < NACT, t * NACT + u, -1)
    pick = (want[:, None] == jnp.arange(NACT * NACT)[None, :]).astype(BF16)
    once = lax.dot_general(pick, rdm, (((1,), (1,)), ((), ())), preferred_element_type=F32).astype(BF16)
    return lax.dot_general(once, pick, (((1,), (1,)), ((), ())), preferred_element_type=F32).astype(BF16)


def per_device(slabs, rdm, orbital_energy, pair_blocks):
    position = lax.axis_index("aux")
    row_block = pair_blocks[position, 0]
    col_block = pair_blocks[position, 1]
    prow, pcol = selectors(col_block)
    r = ordered_rdm(rdm)
    count = lax.axis_size("aux")
    size = count // 2
    half = position // size
    mine = lax.dynamic_slice_in_dim(pair_blocks, half * size, size)
    others = lax.dynamic_slice_in_dim(pair_blocks, (1 - half) * size, size)
    partner_row = others[position % size, 0]

    def shift(block):
        return (block * WIDTH - window_start(block)).reshape(1)

    theirs = exchange(gather(slabs, others), shift(partner_row), 0)
    top = jnp.maximum(jnp.max(jnp.abs(theirs)), F32(1e-30))
    swap = [(i, (i + size) % count) for i in range(count)]
    coded = lax.ppermute((theirs * (1 / top)).astype(jnp.float16), "aux", swap)
    their_top = lax.ppermute(top.reshape(1), "aux", swap)
    kept = exchange(gather(slabs, mine), shift(row_block), 1)
    integrals = (kept + coded.astype(F32) * their_top).astype(BF16)
    raw = pair_sums(integrals, prow, pcol, r)
    paired = raw.reshape(VBLK, 2, HALF).sum(axis=1)[:, :VBLK]
    energy_rows = lax.dynamic_slice_in_dim(orbital_energy, row_block * VBLK, VBLK)
    energy_cols = lax.dynamic_slice_in_dim(orbital_energy, col_block * VBLK, VBLK)
    energy = -paired / (energy_rows[:, None] + energy_cols[None, :])
    weight = jnp.where(row_block == col_block, F32(1.0), F32(2.0))
    total = lax.psum(weight * jnp.sum(energy), "aux")
    mean_energy = total / (VBLK * VBLK * lax.axis_size("aux"))
    return (energy, mean_energy.reshape(1))


def solution(mesh):
    return jax.shard_map(
        per_device,
        mesh=mesh,
        in_specs=(P(("groups", "aux"), None), P("groups", None), P("groups"), P("groups", None)),
        out_specs=(P(("groups", "aux"), None), P("groups")),
        check_vma=False,
    )
```

```python
import functools

import jax
import jax.numpy as jnp
from jax import lax
from jax.experimental import pallas as pl
from jax.experimental.pallas import tpu as pltpu
from jax.sharding import PartitionSpec as P

NACT = 30
VBLK = 48
LANE = 128
HALF = 64
TPAD = 32
WIDTH = VBLK * NACT
WINDOW = -(-(WIDTH + LANE - 32) // LANE) * LANE
UPAIRS = NACT // 2
BF16 = jnp.bfloat16
F32 = jnp.float32


def window_start(block):
    return (block * WIDTH) // LANE * LANE


def gather_body(pairs_ref, in_ref, out_ref):
    out_ref[0] = in_ref[...]


def gather(slabs, pair_blocks):
    rows = slabs.shape[0]
    n = pair_blocks.shape[0]
    return pl.pallas_call(
        gather_body,
        grid_spec=pltpu.PrefetchScalarGridSpec(
            num_scalar_prefetch=1,
            grid=(n, 2),
            in_specs=[
                pl.BlockSpec(
                    (pl.Element(rows), pl.Element(WINDOW)),
                    lambda d, j, pairs: (0, pl.multiple_of(window_start(pairs[d, j]), LANE)),
                )
            ],
            out_specs=pl.BlockSpec((1, rows, WINDOW), lambda d, j, pairs: (d, 0, j)),
        ),
        out_shape=jax.ShapeDtypeStruct((n, rows, 2 * WINDOW), BF16),
        name="gather_blocks",
    )(pair_blocks, slabs)


def exchange_body(size, g_ref, shift_ref, out_ref, recv, acc, local_sem, send_sem, recv_sem):
    position = lax.axis_index("aux")
    base = position // size * size
    me = position - base

    def device(member):
        return {"aux": base + member}

    barrier = pltpu.get_barrier_semaphore()

    @pl.loop(1, size)
    def _(s):
        pl.semaphore_signal(
            barrier, inc=1, device_id=device(lax.rem(me + s, size)), device_id_type=pl.DeviceIdType.MESH
        )

    own = pltpu.make_async_copy(g_ref.at[me], recv.at[me], local_sem)
    own.start()
    pl.semaphore_wait(barrier, size - 1)

    def send(s):
        to = lax.rem(me + s, size)
        return pltpu.make_async_remote_copy(
            src_ref=g_ref.at[to],
            dst_ref=recv.at[me],
            send_sem=send_sem.at[to],
            recv_sem=recv_sem.at[me],
            device_id=device(to),
            device_id_type=pl.DeviceIdType.MESH,
        )

    @pl.loop(1, size)
    def _(s):
        send(s).start()

    acc[...] = jnp.zeros_like(acc)
    own.wait()
    tile = 256

    def add(source):
        @pl.loop(0, WINDOW // tile)
        def _(m):
            at = pl.ds(pl.multiple_of(m * tile, tile), tile)
            acc[at, :] += lax.dot_general(
                recv[source, :, at],
                recv[source, :, WINDOW:],
                (((0,), (0,)), ((), ())),
                preferred_element_type=F32,
            )

    add(me)

    @pl.loop(1, size)
    def _(s):
        source = lax.rem(me + size - s, size)
        pltpu.make_async_remote_copy(
            src_ref=g_ref.at[source],
            dst_ref=recv.at[source],
            send_sem=send_sem.at[source],
            recv_sem=recv_sem.at[source],
            device_id=device(source),
            device_id_type=pl.DeviceIdType.MESH,
        ).wait_recv()
        add(source)

    shift = shift_ref[0]
    piece = 96

    @pl.loop(0, WIDTH // piece)
    def _(m):
        def from_row(offset):
            return acc[pl.ds(pl.multiple_of(m * piece + offset, 32), piece), :]

        low = jnp.where(shift == 0, from_row(0), from_row(32))
        high = jnp.where(shift == 64, from_row(64), from_row(96))
        out_ref[pl.ds(pl.multiple_of(m * piece, 32), piece), :] = jnp.where(shift < 64, low, high)

    @pl.loop(1, size)
    def _(s):
        send(s).wait_send()


def exchange(g, shift, identity):
    size, rows, both = g.shape
    return pl.pallas_call(
        functools.partial(exchange_body, size),
        out_shape=jax.ShapeDtypeStruct((WIDTH, WINDOW), F32),
        in_specs=[pl.BlockSpec(memory_space=pl.ANY), pl.BlockSpec(memory_space=pltpu.SMEM)],
        out_specs=pl.BlockSpec(memory_space=pltpu.VMEM),
        scratch_shapes=[
            pltpu.VMEM((size, rows, both), BF16),
            pltpu.VMEM((WINDOW, WINDOW), F32),
            pltpu.SemaphoreType.DMA,
            pltpu.SemaphoreType.DMA((size,)),
            pltpu.SemaphoreType.DMA((size,)),
        ],
        compiler_params=pltpu.CompilerParams(
            collective_id=identity, has_side_effects=True, vmem_limit_bytes=40 * 2**20
        ),
        cost_estimate=pl.CostEstimate(
            flops=200 * size * rows * WINDOW * WINDOW, bytes_accessed=2 * size * rows * both, transcendentals=0
        ),
        name=f"exchange_blocks_{identity}",
    )(g, shift)


def pair_body(i_ref, prow_ref, pcol_ref, r_ref, out_ref, x_ref):
    tile = 256

    @pl.loop(0, VBLK * TPAD // tile)
    def _(m):
        at = pl.ds(pl.multiple_of(m * tile, tile), tile)
        picked = jnp.dot(prow_ref[at, :], i_ref[...], preferred_element_type=F32).astype(BF16)
        x_ref[at, :] = jnp.dot(picked, pcol_ref[...], preferred_element_type=F32).astype(BF16)

    half = UPAIRS * TPAD

    def stacked(a):
        rows = pl.ds(pl.multiple_of(a * TPAD, TPAD), TPAD)
        return jnp.concatenate([x_ref[rows, u * LANE : (u + 1) * LANE] for u in range(UPAIRS)], axis=0)

    low = lax.broadcasted_iota(jnp.int32, (half, LANE), 1) < HALF

    @pl.loop(0, VBLK // 2)
    def _(m):
        first, second = stacked(2 * m), stacked(2 * m + 1)
        x = jnp.concatenate([first, second], axis=1)
        z0 = jnp.dot(r_ref[:, :half], x, preferred_element_type=F32)
        z1 = jnp.dot(r_ref[:, half:], x, preferred_element_type=F32)
        sums = []
        for k, part in enumerate((first, second)):
            lanes = slice(k * LANE, (k + 1) * LANE)
            xf = part.astype(F32)
            turned = pltpu.roll(xf, HALF, 1)
            b0 = jnp.where(low, xf, turned)
            b1 = jnp.where(low, turned, xf)
            t0 = jnp.where(low, z0[:half, lanes], z1[:half, lanes])
            t1 = jnp.where(low, z0[half:, lanes], z1[half:, lanes])
            sums.append(jnp.sum(t0 * b0 + t1 * b1, axis=0, keepdims=True))
        out_ref[m] = jnp.concatenate(sums, axis=0)


def pair_sums(integrals, prow, pcol, r):
    return pl.pallas_call(
        pair_body,
        out_shape=jax.ShapeDtypeStruct((VBLK // 2, 2, LANE), F32),
        in_specs=[pl.BlockSpec(memory_space=pltpu.VMEM)] * 4,
        out_specs=pl.BlockSpec(memory_space=pltpu.VMEM),
        scratch_shapes=[pltpu.VMEM((VBLK * TPAD, UPAIRS * LANE), BF16)],
        compiler_params=pltpu.CompilerParams(vmem_limit_bytes=48 * 2**20),
        name="pair_sums",
    )(integrals, prow, pcol, r)


def selectors(col_block):
    col_off = col_block * WIDTH - window_start(col_block)
    at = jnp.arange(VBLK * TPAD)
    a, t = at // TPAD, at % TPAD
    want = jnp.where(t < NACT, a * NACT + t, -1)
    prow = (want[:, None] == jnp.arange(WIDTH)[None, :]).astype(BF16)
    j = jnp.arange(UPAIRS * LANE)
    u, b = 2 * (j // LANE) + (j % LANE) // HALF, j % HALF
    want = jnp.where(b < VBLK, col_off + b * NACT + u, -1)
    pcol = (jnp.arange(WINDOW)[:, None] == want[None, :]).astype(BF16)
    return prow, pcol


def ordered_rdm(rdm):
    half = UPAIRS * TPAD
    j = jnp.arange(2 * half)
    u, t = 2 * ((j % half) // TPAD) + j // half, j % TPAD
    want = jnp.where(t < NACT, t * NACT + u, -1)
    pick = (want[:, None] == jnp.arange(NACT * NACT)[None, :]).astype(BF16)
    once = lax.dot_general(pick, rdm, (((1,), (1,)), ((), ())), preferred_element_type=F32).astype(BF16)
    return lax.dot_general(once, pick, (((1,), (1,)), ((), ())), preferred_element_type=F32).astype(BF16)


def per_device(slabs, rdm, orbital_energy, pair_blocks):
    position = lax.axis_index("aux")
    row_block = pair_blocks[position, 0]
    col_block = pair_blocks[position, 1]
    prow, pcol = selectors(col_block)
    r = ordered_rdm(rdm)
    count = lax.axis_size("aux")
    size = count // 2
    half = position // size
    mine = lax.dynamic_slice_in_dim(pair_blocks, half * size, size)
    others = lax.dynamic_slice_in_dim(pair_blocks, (1 - half) * size, size)
    partner_row = others[position % size, 0]

    def shift(block):
        return (block * WIDTH - window_start(block)).reshape(1)

    theirs = exchange(gather(slabs, others), shift(partner_row), 0)
    top = jnp.maximum(jnp.max(jnp.abs(theirs)), F32(1e-30))
    swap = [(i, (i + size) % count) for i in range(count)]
    their_top = lax.ppermute(top.reshape(1), "aux", swap)
    theirs, top, their_top = lax.optimization_barrier((theirs, top, their_top))
    coded = lax.ppermute((theirs * (1 / top)).astype(jnp.float16), "aux", swap)
    kept = exchange(gather(slabs, mine), shift(row_block), 1)
    integrals = (kept + coded.astype(F32) * their_top).astype(BF16)
    raw = pair_sums(integrals, prow, pcol, r)
    paired = raw.reshape(VBLK, 2, HALF).sum(axis=1)[:, :VBLK]
    energy_rows = lax.dynamic_slice_in_dim(orbital_energy, row_block * VBLK, VBLK)
    energy_cols = lax.dynamic_slice_in_dim(orbital_energy, col_block * VBLK, VBLK)
    energy = -paired / (energy_rows[:, None] + energy_cols[None, :])
    weight = jnp.where(row_block == col_block, F32(1.0), F32(2.0))
    total = lax.psum(weight * jnp.sum(energy), "aux")
    mean_energy = total / (VBLK * VBLK * lax.axis_size("aux"))
    return (energy, mean_energy.reshape(1))


def solution(mesh):
    return jax.shard_map(
        per_device,
        mesh=mesh,
        in_specs=(P(("groups", "aux"), None), P("groups", None), P("groups"), P("groups", None)),
        out_specs=(P(("groups", "aux"), None), P("groups")),
        check_vma=False,
    )
```
